32 devices in a mesh: seq: 16 (over z, y, x), head: 2 (over core).
Axes of the slice: x: 2, y: 2, z: 4, core: 2. Of those that a mesh axis runs over, the one named last changes fastest.
Arguments:
- query_vectors: bfloat16 [4096, 2560], P(('seq', 'head')), may hold values from -6 to 6
- address_vectors: bfloat16 [4096, 2560], P(('seq', 'head')), may hold values from -0.75 to 0.75
- payload_vectors: bfloat16 [4096, 2560], P(('seq', 'head')), may hold values from -6 to 6
- forget_logarithms: bfloat16 [4096, 2560], P(('seq', 'head')), may hold values from -1.5 to 0
- pre_sigmoid_filter: bfloat16 [4096, 2560], P(('seq', 'head')), may hold values from -6 to 6
- current_reward_table: float32 [40, 64], replicated, may hold values from -0.5 to 1.5
- cluster_standardize_weight: float32 [2560], replicated, may hold values from 0.25 to 1.75
- cluster_standardize_offset: float32 [2560], replicated, may hold values from -1.5 to 1.5
Outputs:
- mixed: bfloat16 [4096, 2560], P('seq', 'head')
The draws below stay inside these ranges and needn't reach their ends.
All inputs are finite; a program needn't handle non-finite values.
Results may differ from the reference program's by a relative error of at most 0.001.
Values may be sent and summed in bfloat16 or wider, within the bound.
A program may use at most 192 MiB of HBM per device.

```python
import math
import jax
import jax.numpy as jnp
from jax import lax

D = 2560
HOSTED_ATTENDERS = 40
CHANNEL_COUNT = 64
TOK_DEV = 128
TEXT_LENGTH = 4096


def draw_forget_logarithms(key, part):
    address_block = jax.random.split(jax.random.fold_in(key, 17), 7)
    fast_share = 0.5
    element = jax.random.uniform(address_block[3], (TEXT_LENGTH, D), jnp.float32, 0.5, 1.5)
    fast = jax.random.uniform(address_block[0], (HOSTED_ATTENDERS,), jnp.float32) < fast_share
    slow_rate = jnp.exp(jax.random.uniform(address_block[1], (HOSTED_ATTENDERS, CHANNEL_COUNT), jnp.float32, math.log(0.2), math.log(0.8))) / TEXT_LENGTH
    fast_rate = jnp.exp(jax.random.uniform(address_block[2], (HOSTED_ATTENDERS, CHANNEL_COUNT), jnp.float32, math.log(1.0 / 50.0), math.log(1.0 / 25.0)))
    forget_speed = jnp.where(fast[:, None], fast_rate, slow_rate).reshape(D)
    slabs = TEXT_LENGTH // TOK_DEV
    slab_factor = jax.random.uniform(address_block[4], (slabs, 1, 1), jnp.float32, 0.6, 1.5)
    forget_weighting = (element.reshape(slabs, TOK_DEV, D) * slab_factor).reshape(TEXT_LENGTH, D)
    block_offsets = jax.random.randint(address_block[5], (3,), 0, TEXT_LENGTH)
    forget_shrinkage = jax.random.uniform(address_block[6], (3,), jnp.float32, 0.2, 0.35)
    word_spans = jnp.zeros((TEXT_LENGTH,), jnp.float32).at[block_offsets].add(-jnp.log(1.0 - forget_shrinkage))
    return (-(forget_speed[None, :] * forget_weighting) - word_spans[:, None]).astype(jnp.bfloat16)


def steps_of(key, extent, cuts, low, top_value):
    loudness, own = 1.0, jax.random.fold_in(key, 6)
    for axis_at, shards_of in cuts:
        heights = jnp.exp(jax.random.uniform(jax.random.fold_in(own, axis_at), (shards_of,), jnp.float32, low / len(cuts), top_value / len(cuts)))
        loudness = loudness * jnp.repeat(heights, extent[axis_at] // shards_of).reshape([-1 if axis == axis_at else 1 for axis in range(len(extent))])
    return loudness


def centred(key, shape, width, bound, cuts=(), dtype=jnp.bfloat16):
    entries = jax.random.normal(key, shape, jnp.float32) * width
    if len(cuts) > 0:
        entries = steps_of(key, shape, cuts, -0.22, 0.18) * entries
    return jnp.clip(entries, min=-bound, max=bound).astype(dtype)


def setup_inputs(seed: int = 0) -> dict:
    streams_of = jax.random.split(jax.random.key(seed), 9)
    query_vectors = centred(streams_of[0], (TEXT_LENGTH, D), 1.0, 6.0, ((0, 32),))
    address_vectors = centred(streams_of[1], (TEXT_LENGTH, D), 0.125, 0.75, ((0, 32),))
    payload_vectors = centred(streams_of[2], (TEXT_LENGTH, D), 1.0, 6.0, ((0, 32),))
    forget_logarithms = draw_forget_logarithms(jax.random.fold_in(streams_of[8], 71), 0)
    pre_sigmoid_filter = centred(streams_of[4], (TEXT_LENGTH, D), 1.0, 6.0, ((0, 32),))
    current_reward_table = jnp.clip(jax.random.uniform(streams_of[5], (HOSTED_ATTENDERS, CHANNEL_COUNT), jnp.float32, -0.5, 1.5), -0.5, 1.5)
    cluster_standardize_weight = jnp.clip(1.0 + 0.15 * jax.random.normal(streams_of[6], (D,), jnp.float32), 0.25, 1.75)
    cluster_standardize_offset = centred(streams_of[7], (D,), 0.3, 1.5, (), jnp.float32)
    return dict(query_vectors=query_vectors, address_vectors=address_vectors, payload_vectors=payload_vectors, forget_logarithms=forget_logarithms, pre_sigmoid_filter=pre_sigmoid_filter, current_reward_table=current_reward_table, cluster_standardize_weight=cluster_standardize_weight, cluster_standardize_offset=cluster_standardize_offset)


def reference(query_vectors, address_vectors, payload_vectors, forget_logarithms, pre_sigmoid_filter, current_reward_table, cluster_standardize_weight, cluster_standardize_offset):
    highest = lax.Precision.HIGHEST
    blocks = TEXT_LENGTH // TOK_DEV

    def prepare(array):
        return array.astype(jnp.float32).reshape(blocks, TOK_DEV, HOSTED_ATTENDERS, CHANNEL_COUNT)
    later = lax.broadcasted_iota(jnp.int32, (TOK_DEV, TOK_DEV), 0)
    earlier = lax.broadcasted_iota(jnp.int32, (TOK_DEV, TOK_DEV), 1)
    strict = later > earlier

    def advance(state, pieces):
        incoming_memory, address_block, payload_block, forget_multiplier = pieces
        cumul = jnp.cumsum(forget_multiplier, axis=0)
        before = cumul - forget_multiplier
        final = cumul[-1]
        scaled_receptance = incoming_memory * jnp.exp(before)
        scaled_k = address_block * jnp.exp(-cumul)
        end_keys = address_block * jnp.exp(final[None] - cumul)
        scores = jnp.einsum('thc,shc->hts', scaled_receptance, scaled_k, precision=highest)
        scores = jnp.where(strict[None], scores, jnp.float32(0.0))
        diagonal_piece = lax.optimization_barrier(jnp.sum(incoming_memory * current_reward_table[None] * address_block, axis=2))
        mixed_output = jnp.einsum('hts,shj->thj', scores, payload_block, precision=highest)
        mixed_output = mixed_output + jnp.einsum('thc,hcj->thj', scaled_receptance, state, precision=highest)
        mixed_output = mixed_output + diagonal_piece[:, :, None] * payload_block
        state = jnp.exp(final)[:, :, None] * state + jnp.einsum('shc,shj->hcj', end_keys, payload_block, precision=highest)
        return (state, mixed_output)
    start_state = jnp.zeros((HOSTED_ATTENDERS, CHANNEL_COUNT, CHANNEL_COUNT), jnp.float32)
    _, outputs = lax.scan(advance, start_state, (prepare(query_vectors), prepare(address_vectors), prepare(payload_vectors), prepare(forget_logarithms)))
    outputs = outputs.reshape(TEXT_LENGTH, HOSTED_ATTENDERS, CHANNEL_COUNT)
    center = outputs - lax.optimization_barrier(jnp.mean(outputs, axis=2, keepdims=True))
    spread = lax.optimization_barrier(jnp.mean(center * center, axis=2, keepdims=True))
    normed = (center * lax.rsqrt(spread + 1e-05)).reshape(TEXT_LENGTH, D)
    gate = pre_sigmoid_filter.astype(jnp.float32)
    return ((normed * cluster_standardize_weight[None] + cluster_standardize_offset[None]) * gate * jax.nn.sigmoid(gate)).astype(jnp.bfloat16)
```

```python
import functools

import jax
import jax.numpy as jnp
from jax import lax
from jax.experimental import pallas as pl
from jax.experimental.pallas import tpu as pltpu
from jax.sharding import PartitionSpec as P

CHANNEL_COUNT = 64
PAIR = 2 * CHANNEL_COUNT
ROWS = 8
MESH = pl.DeviceIdType.MESH
BF = jnp.bfloat16
F32 = jnp.float32


def split(x):
    high = x.astype(BF)
    return high, (x - high.astype(F32)).astype(BF)


def dot(a, b):
    return jnp.dot(a, b, preferred_element_type=F32)


def dot_nt(a, b):
    return lax.dot_general(a, b, (((1,), (1,)), ((), ())), preferred_element_type=F32)


def dot_tn(a, b):
    return lax.dot_general(a, b, (((0,), (0,)), ((), ())), preferred_element_type=F32)


def kernel(
    n,
    heads,
    units,
    q_hbm,
    k_hbm,
    v_hbm,
    w_hbm,
    g_hbm,
    bonus_ref,
    gain_ref,
    bias_ref,
    out_ref,
    xq,
    xk,
    xv,
    xw,
    xg,
    rhi_ref,
    rlo_ref,
    khi_ref,
    klo_ref,
    y_ref,
    local_ref,
    small_ref,
    msg,
    inbox,
    prefix,
    carried,
    local_sem,
    hsend,
    hrecv,
    send1,
    recv1,
    send2,
    recv2,
):
    me, half = lax.axis_index("seq"), lax.axis_index("head")
    rows, width = q_hbm.shape[0], out_ref.shape[1]
    pairs = width // PAIR
    groups = CHANNEL_COUNT // ROWS
    unit_rows = units * ROWS
    sources = (w_hbm, k_hbm, v_hbm, q_hbm, g_hbm)
    targets = (xw, xk, xv, xq, xg)

    barrier = pltpu.get_barrier_semaphore()
    for step in range(1, heads):
        other = lax.rem(half + step, heads)
        pl.semaphore_signal(barrier, inc=1, device_id=(me, other), device_id_type=MESH)

    def greet(step, carry):
        peer = lax.rem(me + step, n)
        pl.semaphore_signal(barrier, inc=1, device_id=(peer, half), device_id_type=MESH)
        return carry

    lax.fori_loop(1, n, greet, 0)

    mine = pl.ds(pl.multiple_of(half * rows, rows), rows)
    locals_ = []
    for at, (source, target) in enumerate(zip(sources, targets)):
        copy = pltpu.make_async_copy(
            source.at[:, pl.ds(pl.multiple_of(half * width, PAIR), width)],
            target.at[mine, :],
            local_sem.at[at],
        )
        copy.start()
        locals_.append(copy)
    pl.semaphore_wait(barrier, n - 1 + heads - 1)
    remotes = []
    for at, (source, target) in enumerate(zip(sources, targets)):
        group = []
        for step in range(1, heads):
            other = lax.rem(half + step, heads)
            copy = pltpu.make_async_remote_copy(
                src_ref=source.at[:, pl.ds(pl.multiple_of(other * width, PAIR), width)],
                dst_ref=target.at[mine, :],
                send_sem=hsend.at[at, step - 1],
                recv_sem=hrecv.at[at, step - 1],
                device_id=(me, other),
                device_id_type=MESH,
            )
            copy.start()
            group.append(copy)
        remotes.append(group)

    def arrived(at):
        locals_[at].wait()
        for copy in remotes[at]:
            copy.wait_recv()

    lower = (
        lax.broadcasted_iota(jnp.int32, (rows, rows), 0)
        >= lax.broadcasted_iota(jnp.int32, (rows, rows), 1)
    ).astype(F32).astype(BF)
    lane = lax.broadcasted_iota(jnp.int32, (1, PAIR), 1)
    first_f = (lane < CHANNEL_COUNT).astype(F32)
    second_f = 1.0 - first_f
    first, second = first_f.astype(BF), second_f.astype(BF)
    at_row = lax.broadcasted_iota(jnp.int32, (2 * PAIR, PAIR), 0)
    at_lane = lax.broadcasted_iota(jnp.int32, (2 * PAIR, PAIR), 1)
    ones = (
        (lax.rem(at_row, PAIR) < CHANNEL_COUNT) == (at_lane < CHANNEL_COUNT)
    ).astype(F32).astype(BF)

    def head_sums(x):
        return dot(jnp.concatenate(split(x), axis=1), ones)

    for spare in range(pairs * groups, n * units):
        msg[spare // units, (spare % units) * ROWS : (spare % units + 1) * ROWS] = jnp.zeros(
            (ROWS, PAIR), F32
        )

    def spot(chunk, pair):
        return slice(chunk * rows, (chunk + 1) * rows), slice(pair * PAIR, (pair + 1) * PAIR)

    def summarize(pair):
        state = total = None
        for chunk in range(heads):
            at = spot(chunk, pair)
            decay = xw[at]
            cumul = dot(lower, decay)
            final = cumul[rows - 1 : rows]
            center = 0.5 * final
            high, low = split(xq[at].astype(F32) * jnp.exp(cumul - decay.astype(F32) - center))
            rhi_ref[at], rlo_ref[at] = high, low
            high, low = split(xk[at].astype(F32) * jnp.exp(center - cumul))
            khi_ref[at], klo_ref[at] = high, low
            full = dot_tn(xv[at], jnp.concatenate([high, low], axis=1))
            full = full[:, :PAIR] + full[:, PAIR:]
            scale = jnp.exp(center)
            ends = jnp.where(lane < CHANNEL_COUNT, full[:CHANNEL_COUNT], full[CHANNEL_COUNT:])
            ends = ends * scale
            step = jnp.exp(final)
            small_ref[2 * chunk : 2 * chunk + 1, at[1]] = scale
            if chunk == 0:
                state, total = ends, step
            else:
                small_ref[2 * chunk + 1 : 2 * chunk + 2, at[1]] = total
                local_ref[chunk - 1, pair] = state
                state, total = step * state + ends, step * total
        for group in range(groups):
            unit = pair * groups + group
            to, slot = unit // units, unit % units
            msg[to, slot * ROWS : (slot + 1) * ROWS] = state[group * ROWS : (group + 1) * ROWS]
            msg[to, unit_rows + slot : unit_rows + slot + 1] = total

    def within(pair):
        bonus = bonus_ref[
            :, pl.ds(pl.multiple_of(half * width + pair * PAIR, PAIR), PAIR)
        ]
        for chunk in range(heads):
            at = spot(chunk, pair)
            high, low = rhi_ref[at], rlo_ref[at]
            key_high, key_low, value = khi_ref[at], klo_ref[at], xv[at]
            keys = jnp.concatenate([key_high * first, key_high * second], axis=0)
            rest = jnp.concatenate([key_low * first, key_low * second], axis=0)
            scores = dot_nt(
                jnp.concatenate([high, low], axis=1), jnp.concatenate([keys, keys], axis=1)
            ) + dot_nt(high, rest)
            strict = lax.broadcasted_iota(jnp.int32, scores.shape, 0) > lax.rem(
                lax.broadcasted_iota(jnp.int32, scores.shape, 1), rows
            )
            scores = jnp.where(strict, scores, 0.0)
            values = jnp.concatenate([value * first, value * second], axis=0)
            both = dot(jnp.concatenate(split(scores), axis=0), values)
            diagonal = head_sums(xq[at].astype(F32) * bonus * xk[at].astype(F32))
            y_ref[at] = both[:rows] + both[rows:] + diagonal * value.astype(F32)

    def finish(pair):
        lanes = pl.ds(pl.multiple_of(half * width + pair * PAIR, PAIR), PAIR)
        gain, bias = gain_ref[:, lanes], bias_ref[:, lanes]
        pieces = []
        for group in range(groups):
            unit = pair * groups + group
            slot = unit % units
            pieces.append(carried[unit // units, slot * ROWS : (slot + 1) * ROWS])
        incoming = jnp.concatenate(pieces, axis=0)
        for chunk in range(heads):
            at = spot(chunk, pair)
            state = incoming
            if chunk > 0:
                total = small_ref[2 * chunk + 1 : 2 * chunk + 2, at[1]]
                state = total * incoming + local_ref[chunk - 1, pair]
            state = state * small_ref[2 * chunk : 2 * chunk + 1, at[1]]
            state_high, state_low = split(
                jnp.concatenate([state * first_f, state * second_f], axis=0)
            )
            high, low = rhi_ref[at], rlo_ref[at]
            y = (
                y_ref[at]
                + dot_nt(
                    jnp.concatenate([high, low], axis=1),
                    jnp.concatenate([state_high, state_high], axis=1),
                )
                + dot_nt(high, state_low)
            )
            y = y - head_sums(y) * (1.0 / CHANNEL_COUNT)
            spread = head_sums(y * y) * (1.0 / CHANNEL_COUNT)
            normed = y * lax.rsqrt(spread + 1e-05)
            gate = xg[at].astype(F32)
            gated = (normed * gain + bias) * (gate / (1.0 + jnp.exp(-gate)))
            out_ref[at] = gated.astype(out_ref.dtype)

    def outgoing(peer):
        return pltpu.make_async_remote_copy(
            src_ref=msg.at[peer],
            dst_ref=inbox.at[me],
            send_sem=send1.at[peer],
            recv_sem=recv1.at[me],
            device_id=(peer, half),
            device_id_type=MESH,
        )

    def incoming_from(peer):
        return pltpu.make_async_remote_copy(
            src_ref=msg.at[peer],
            dst_ref=inbox.at[peer],
            send_sem=send1.at[peer],
            recv_sem=recv1.at[peer],
            device_id=(peer, half),
            device_id_type=MESH,
        )

    def back_to(peer):
        return pltpu.make_async_remote_copy(
            src_ref=prefix.at[peer],
            dst_ref=carried.at[me],
            send_sem=send2.at[peer],
            recv_sem=recv2.at[me],
            device_id=(peer, half),
            device_id_type=MESH,
        )

    def back_from(peer):
        return pltpu.make_async_remote_copy(
            src_ref=prefix.at[peer],
            dst_ref=carried.at[peer],
            send_sem=send2.at[peer],
            recv_sem=recv2.at[peer],
            device_id=(peer, half),
            device_id_type=MESH,
        )

    def others(act):
        def body(step, carry):
            act(lax.rem(me + step, n))
            return carry

        lax.fori_loop(1, n, body, 0)

    for at in range(4):
        arrived(at)
    for pair in range(pairs):
        summarize(pair)
    others(lambda peer: outgoing(peer).start())
    inbox[me] = msg[me]
    early = pairs // 2
    for pair in range(early):
        within(pair)

    def scan(source, state):
        prefix[source] = state

        @pl.when(source != me)
        def _():
            back_to(source).start()

        @pl.when(source == me)
        def _():
            carried[source] = state

        @pl.when(source != me)
        def _():
            incoming_from(source).wait_recv()

        block = inbox[source]
        parts = []
        for slot in range(units):
            rows_of = slice(slot * ROWS, (slot + 1) * ROWS)
            decay = block[unit_rows + slot : unit_rows + slot + 1]
            parts.append(state[rows_of] * decay + block[rows_of])
        return jnp.concatenate(parts, axis=0) if units > 1 else parts[0]

    lax.fori_loop(0, n, scan, jnp.zeros((unit_rows, PAIR), F32))
    for pair in range(early, pairs):
        within(pair)
    arrived(4)
    others(lambda peer: back_from(peer).wait_recv())
    for pair in range(pairs):
        finish(pair)
    for group in remotes:
        for copy in group:
            copy.wait_send()
    others(lambda peer: outgoing(peer).wait_send())
    others(lambda peer: back_to(peer).wait_send())


def solution(mesh):
    n, heads = mesh.shape["seq"], mesh.shape["head"]

    def body(q, k, v, w, g, bonus, gain, bias):
        rows, full = q.shape
        width = full // heads
        length = rows * heads
        pairs = width // PAIR
        units = -(-pairs * (CHANNEL_COUNT // ROWS) // n)
        unit_rows = units * ROWS
        message_rows = unit_rows + -(-units // ROWS) * ROWS
        anywhere = pl.BlockSpec(memory_space=pl.ANY)
        inside = pl.BlockSpec(memory_space=pltpu.VMEM)
        dma = pltpu.SemaphoreType.DMA
        slab = (length, width)
        return pl.pallas_call(
            functools.partial(kernel, n, heads, units),
            out_shape=jax.ShapeDtypeStruct(slab, jnp.bfloat16),
            in_specs=[anywhere] * 5 + [inside] * 3,
            out_specs=inside,
            scratch_shapes=[pltpu.VMEM(slab, BF)] * 9
            + [
                pltpu.VMEM(slab, F32),
                pltpu.VMEM((max(heads - 1, 1), pairs, CHANNEL_COUNT, PAIR), F32),
                pltpu.VMEM((2 * heads, width), F32),
                pltpu.VMEM((n, message_rows, PAIR), F32),
                pltpu.VMEM((n, message_rows, PAIR), F32),
                pltpu.VMEM((n, unit_rows, PAIR), F32),
                pltpu.VMEM((n, unit_rows, PAIR), F32),
                dma((5,)),
                dma((5, max(heads - 1, 1))),
                dma((5, max(heads - 1, 1))),
                dma((n,)),
                dma((n,)),
                dma((n,)),
                dma((n,)),
            ],
            compiler_params=pltpu.CompilerParams(
                collective_id=0, has_side_effects=True, vmem_limit_bytes=40 * 1024 * 1024
            ),
        )(q, k, v, w, g, bonus.reshape(1, full), gain.reshape(1, full), bias.reshape(1, full))

    slabs = P(("seq", "head"), None)
    return jax.shard_map(
        body,
        mesh=mesh,
        in_specs=(slabs,) * 5 + (P(), P(), P()),
        out_specs=P("seq", "head"),
        check_vma=False,
    )
```

```python
import functools

import jax
import jax.numpy as jnp
from jax import lax
from jax.experimental import pallas as pl
from jax.experimental.pallas import tpu as pltpu
from jax.sharding import PartitionSpec as P

CHANNEL_COUNT = 64
PAIR = 2 * CHANNEL_COUNT
ROWS = 8
MESH = pl.DeviceIdType.MESH
BF = jnp.bfloat16
F32 = jnp.float32


def split(x):
    high = x.astype(BF)
    return high, (x - high.astype(F32)).astype(BF)


def dot(a, b):
    return jnp.dot(a, b, preferred_element_type=F32)


def dot_nt(a, b):
    return lax.dot_general(a, b, (((1,), (1,)), ((), ())), preferred_element_type=F32)


def dot_tn(a, b):
    return lax.dot_general(a, b, (((0,), (0,)), ((), ())), preferred_element_type=F32)


def kernel(
    n,
    heads,
    units,
    q_hbm,
    k_hbm,
    v_hbm,
    w_hbm,
    g_hbm,
    bonus_hbm,
    gain_hbm,
    bias_hbm,
    out_ref,
    bonus_ref,
    gain_ref,
    bias_ref,
    xq,
    xk,
    xv,
    xw,
    xg,
    rhi_ref,
    rlo_ref,
    khi_ref,
    klo_ref,
    y_ref,
    local_ref,
    small_ref,
    msg,
    inbox,
    prefix,
    carried,
    local_sem,
    hsend,
    hrecv,
    send1,
    recv1,
    send2,
    recv2,
):
    me, half = lax.axis_index("seq"), lax.axis_index("head")
    rows, width = q_hbm.shape[0], out_ref.shape[1]
    pairs = width // PAIR
    groups = CHANNEL_COUNT // ROWS
    unit_rows = units * ROWS
    sources = (w_hbm, k_hbm, v_hbm, q_hbm, g_hbm)
    targets = (xw, xk, xv, xq, xg)

    barrier = pltpu.get_barrier_semaphore()
    for step in range(1, heads):
        other = lax.rem(half + step, heads)
        pl.semaphore_signal(barrier, inc=1, device_id=(me, other), device_id_type=MESH)

    def greet(step, carry):
        peer = lax.rem(me + step, n)
        pl.semaphore_signal(barrier, inc=1, device_id=(peer, half), device_id_type=MESH)
        return carry

    lax.fori_loop(1, n, greet, 0)

    mine = pl.ds(pl.multiple_of(half * rows, rows), rows)
    locals_ = []
    for at, (source, target) in enumerate(zip(sources, targets)):
        copy = pltpu.make_async_copy(
            source.at[:, pl.ds(pl.multiple_of(half * width, PAIR), width)],
            target.at[mine, :],
            local_sem.at[at],
        )
        copy.start()
        locals_.append(copy)
    params = []
    for at, (source, target) in enumerate(
        ((bonus_hbm, bonus_ref), (gain_hbm, gain_ref), (bias_hbm, bias_ref))
    ):
        copy = pltpu.make_async_copy(source, target, local_sem.at[5 + at])
        copy.start()
        params.append(copy)
    pl.semaphore_wait(barrier, n - 1 + heads - 1)
    remotes = []
    for at, (source, target) in enumerate(zip(sources, targets)):
        group = []
        for step in range(1, heads):
            other = lax.rem(half + step, heads)
            copy = pltpu.make_async_remote_copy(
                src_ref=source.at[:, pl.ds(pl.multiple_of(other * width, PAIR), width)],
                dst_ref=target.at[mine, :],
                send_sem=hsend.at[at, step - 1],
                recv_sem=hrecv.at[at, step - 1],
                device_id=(me, other),
                device_id_type=MESH,
            )
            copy.start()
            group.append(copy)
        remotes.append(group)

    def arrived(at):
        locals_[at].wait()
        for copy in remotes[at]:
            copy.wait_recv()

    lower = (
        lax.broadcasted_iota(jnp.int32, (rows, rows), 0)
        >= lax.broadcasted_iota(jnp.int32, (rows, rows), 1)
    ).astype(F32).astype(BF)
    lane = lax.broadcasted_iota(jnp.int32, (1, PAIR), 1)
    first_f = (lane < CHANNEL_COUNT).astype(F32)
    second_f = 1.0 - first_f
    first, second = first_f.astype(BF), second_f.astype(BF)
    at_row = lax.broadcasted_iota(jnp.int32, (2 * PAIR, PAIR), 0)
    at_lane = lax.broadcasted_iota(jnp.int32, (2 * PAIR, PAIR), 1)
    ones = (
        (lax.rem(at_row, PAIR) < CHANNEL_COUNT) == (at_lane < CHANNEL_COUNT)
    ).astype(F32).astype(BF)

    def head_sums(x):
        return dot(jnp.concatenate(split(x), axis=1), ones)

    for spare in range(pairs * groups, n * units):
        msg[spare // units, (spare % units) * ROWS : (spare % units + 1) * ROWS] = jnp.zeros(
            (ROWS, PAIR), F32
        )

    def spot(chunk, pair):
        return slice(chunk * rows, (chunk + 1) * rows), slice(pair * PAIR, (pair + 1) * PAIR)

    def summarize(pair):
        state = total = None
        for chunk in range(heads):
            at = spot(chunk, pair)
            decay = xw[at]
            cumul = dot(lower, decay)
            final = cumul[rows - 1 : rows]
            center = 0.5 * final
            high, low = split(xq[at].astype(F32) * jnp.exp(cumul - decay.astype(F32) - center))
            rhi_ref[at], rlo_ref[at] = high, low
            high, low = split(xk[at].astype(F32) * jnp.exp(center - cumul))
            khi_ref[at], klo_ref[at] = high, low
            full = dot_tn(xv[at], jnp.concatenate([high, low], axis=1))
            full = full[:, :PAIR] + full[:, PAIR:]
            scale = jnp.exp(center)
            ends = jnp.where(lane < CHANNEL_COUNT, full[:CHANNEL_COUNT], full[CHANNEL_COUNT:])
            ends = ends * scale
            step = jnp.exp(final)
            small_ref[2 * chunk : 2 * chunk + 1, at[1]] = scale
            if chunk == 0:
                state, total = ends, step
            else:
                small_ref[2 * chunk + 1 : 2 * chunk + 2, at[1]] = total
                local_ref[chunk - 1, pair] = state
                state, total = step * state + ends, step * total
        for group in range(groups):
            unit = pair * groups + group
            to, slot = unit // units, unit % units
            msg[to, slot * ROWS : (slot + 1) * ROWS] = state[group * ROWS : (group + 1) * ROWS]
            msg[to, unit_rows + slot : unit_rows + slot + 1] = total

    def within(pair):
        head = half * (width // CHANNEL_COUNT) + 2 * pair
        bonus = jnp.concatenate([bonus_ref[pl.ds(head, 1)], bonus_ref[pl.ds(head + 1, 1)]], axis=1)
        for chunk in range(heads):
            at = spot(chunk, pair)
            high, low = rhi_ref[at], rlo_ref[at]
            key_high, key_low, value = khi_ref[at], klo_ref[at], xv[at]
            keys = jnp.concatenate([key_high * first, key_high * second], axis=0)
            rest = jnp.concatenate([key_low * first, key_low * second], axis=0)
            scores = dot_nt(
                jnp.concatenate([high, low], axis=1), jnp.concatenate([keys, keys], axis=1)
            ) + dot_nt(high, rest)
            strict = lax.broadcasted_iota(jnp.int32, scores.shape, 0) > lax.rem(
                lax.broadcasted_iota(jnp.int32, scores.shape, 1), rows
            )
            scores = jnp.where(strict, scores, 0.0)
            values = jnp.concatenate([value * first, value * second], axis=0)
            both = dot(jnp.concatenate(split(scores), axis=0), values)
            diagonal = head_sums(xq[at].astype(F32) * bonus * xk[at].astype(F32))
            y_ref[at] = both[:rows] + both[rows:] + diagonal * value.astype(F32)

    def finish(pair):
        lanes = pl.ds(pl.multiple_of(half * width + pair * PAIR, PAIR), PAIR)
        gain, bias = gain_ref[lanes].reshape(1, PAIR), bias_ref[lanes].reshape(1, PAIR)
        pieces = []
        for group in range(groups):
            unit = pair * groups + group
            slot = unit % units
            pieces.append(carried[unit // units, slot * ROWS : (slot + 1) * ROWS])
        incoming = jnp.concatenate(pieces, axis=0)
        for chunk in range(heads):
            at = spot(chunk, pair)
            state = incoming
            if chunk > 0:
                total = small_ref[2 * chunk + 1 : 2 * chunk + 2, at[1]]
                state = total * incoming + local_ref[chunk - 1, pair]
            state = state * small_ref[2 * chunk : 2 * chunk + 1, at[1]]
            state_high, state_low = split(
                jnp.concatenate([state * first_f, state * second_f], axis=0)
            )
            high, low = rhi_ref[at], rlo_ref[at]
            y = (
                y_ref[at]
                + dot_nt(
                    jnp.concatenate([high, low], axis=1),
                    jnp.concatenate([state_high, state_high], axis=1),
                )
                + dot_nt(high, state_low)
            )
            y = y - head_sums(y) * (1.0 / CHANNEL_COUNT)
            spread = head_sums(y * y) * (1.0 / CHANNEL_COUNT)
            normed = y * lax.rsqrt(spread + 1e-05)
            gate = xg[at].astype(F32)
            gated = (normed * gain + bias) * (gate / (1.0 + jnp.exp(-gate)))
            out_ref[at] = gated.astype(out_ref.dtype)

    def outgoing(peer):
        return pltpu.make_async_remote_copy(
            src_ref=msg.at[peer],
            dst_ref=inbox.at[me],
            send_sem=send1.at[peer],
            recv_sem=recv1.at[me],
            device_id=(peer, half),
            device_id_type=MESH,
        )

    def incoming_from(peer):
        return pltpu.make_async_remote_copy(
            src_ref=msg.at[peer],
            dst_ref=inbox.at[peer],
            send_sem=send1.at[peer],
            recv_sem=recv1.at[peer],
            device_id=(peer, half),
            device_id_type=MESH,
        )

    def back_to(peer):
        return pltpu.make_async_remote_copy(
            src_ref=prefix.at[peer],
            dst_ref=carried.at[me],
            send_sem=send2.at[peer],
            recv_sem=recv2.at[me],
            device_id=(peer, half),
            device_id_type=MESH,
        )

    def back_from(peer):
        return pltpu.make_async_remote_copy(
            src_ref=prefix.at[peer],
            dst_ref=carried.at[peer],
            send_sem=send2.at[peer],
            recv_sem=recv2.at[peer],
            device_id=(peer, half),
            device_id_type=MESH,
        )

    def others(act):
        def body(step, carry):
            act(lax.rem(me + step, n))
            return carry

        lax.fori_loop(1, n, body, 0)

    for at in range(4):
        arrived(at)
    for pair in range(pairs):
        summarize(pair)
    others(lambda peer: outgoing(peer).start())
    for copy in params:
        copy.wait()
    inbox[me] = msg[me]
    early = pairs // 2
    for pair in range(early):
        within(pair)

    def scan(source, state):
        prefix[source] = state

        @pl.when(source != me)
        def _():
            back_to(source).start()

        @pl.when(source == me)
        def _():
            carried[source] = state

        @pl.when(source != me)
        def _():
            incoming_from(source).wait_recv()

        block = inbox[source]
        parts = []
        for slot in range(units):
            rows_of = slice(slot * ROWS, (slot + 1) * ROWS)
            decay = block[unit_rows + slot : unit_rows + slot + 1]
            parts.append(state[rows_of] * decay + block[rows_of])
        return jnp.concatenate(parts, axis=0) if units > 1 else parts[0]

    lax.fori_loop(0, n, scan, jnp.zeros((unit_rows, PAIR), F32))
    for pair in range(early, pairs):
        within(pair)
    arrived(4)
    others(lambda peer: back_from(peer).wait_recv())
    for pair in range(pairs):
        finish(pair)
    for group in remotes:
        for copy in group:
            copy.wait_send()
    others(lambda peer: outgoing(peer).wait_send())
    others(lambda peer: back_to(peer).wait_send())


def solution(mesh):
    n, heads = mesh.shape["seq"], mesh.shape["head"]

    def body(q, k, v, w, g, bonus, gain, bias):
        rows, full = q.shape
        width = full // heads
        length = rows * heads
        pairs = width // PAIR
        units = -(-pairs * (CHANNEL_COUNT // ROWS) // n)
        unit_rows = units * ROWS
        message_rows = unit_rows + -(-units // ROWS) * ROWS
        anywhere = pl.BlockSpec(memory_space=pltpu.HBM)
        inside = pl.BlockSpec(memory_space=pltpu.VMEM)
        dma = pltpu.SemaphoreType.DMA
        slab = (length, width)
        return pl.pallas_call(
            functools.partial(kernel, n, heads, units),
            out_shape=jax.ShapeDtypeStruct(slab, jnp.bfloat16),
            in_specs=[anywhere] * 8,
            out_specs=inside,
            scratch_shapes=[pltpu.VMEM(bonus.shape, F32)]
            + [pltpu.VMEM((full,), F32)] * 2
            + [pltpu.VMEM(slab, BF)] * 9
            + [
                pltpu.VMEM(slab, F32),
                pltpu.VMEM((max(heads - 1, 1), pairs, CHANNEL_COUNT, PAIR), F32),
                pltpu.VMEM((2 * heads, width), F32),
                pltpu.VMEM((n, message_rows, PAIR), F32),
                pltpu.VMEM((n, message_rows, PAIR), F32),
                pltpu.VMEM((n, unit_rows, PAIR), F32),
                pltpu.VMEM((n, unit_rows, PAIR), F32),
                dma((8,)),
                dma((5, max(heads - 1, 1))),
                dma((5, max(heads - 1, 1))),
                dma((n,)),
                dma((n,)),
                dma((n,)),
                dma((n,)),
            ],
            compiler_params=pltpu.CompilerParams(
                collective_id=0, has_side_effects=True, vmem_limit_bytes=60 * 1024 * 1024
            ),
        )(q, k, v, w, g, bonus, gain, bias)

    slabs = P(("seq", "head"), None)
    return jax.shard_map(
        body,
        mesh=mesh,
        in_specs=(slabs,) * 5 + (P(), P(), P()),
        out_specs=P("seq", "head"),
        check_vma=False,
    )
```

```python
import functools

import jax
import jax.numpy as jnp
from jax import lax
from jax.experimental import pallas as pl
from jax.experimental.pallas import tpu as pltpu
from jax.sharding import PartitionSpec as P

CHANNEL_COUNT = 64
PAIR = 2 * CHANNEL_COUNT
ROWS = 8
MESH = pl.DeviceIdType.MESH
BF = jnp.bfloat16
F32 = jnp.float32


def split(x):
    high = x.astype(BF)
    return high, (x - high.astype(F32)).astype(BF)


def dot(a, b):
    return jnp.dot(a, b, preferred_element_type=F32)


def dot_nt(a, b):
    return lax.dot_general(a, b, (((1,), (1,)), ((), ())), preferred_element_type=F32)


def dot_tn(a, b):
    return lax.dot_general(a, b, (((0,), (0,)), ((), ())), preferred_element_type=F32)


def kernel(
    n,
    heads,
    units,
    q_hbm,
    k_hbm,
    v_hbm,
    w_hbm,
    g_hbm,
    bonus_hbm,
    gain_hbm,
    bias_hbm,
    out_ref,
    bonus_ref,
    gain_ref,
    bias_ref,
    xq,
    xk,
    xv,
    xw,
    xg,
    own_w,
    own_k,
    own_v,
    ends_out,
    ends_in,
    rhi_ref,
    rlo_ref,
    khi_ref,
    klo_ref,
    y_ref,
    local_ref,
    small_ref,
    msg,
    inbox,
    prefix,
    carried,
    local_sem,
    esend,
    erecv,
    hsend,
    hrecv,
    send1,
    recv1,
    send2,
    recv2,
):
    me, half = lax.axis_index("seq"), lax.axis_index("head")
    rows, width = q_hbm.shape[0], out_ref.shape[1]
    pairs = width // PAIR
    groups = CHANNEL_COUNT // ROWS
    unit_rows = units * ROWS
    sources = (w_hbm, k_hbm, v_hbm, q_hbm, g_hbm)
    targets = (xw, xk, xv, xq, xg)

    barrier = pltpu.get_barrier_semaphore()
    for step in range(1, heads):
        other = lax.rem(half + step, heads)
        pl.semaphore_signal(barrier, inc=1, device_id=(me, other), device_id_type=MESH)

    def greet(step, carry):
        peer = lax.rem(me + step, n)
        pl.semaphore_signal(barrier, inc=1, device_id=(peer, half), device_id_type=MESH)
        return carry

    lax.fori_loop(1, n, greet, 0)

    mine = pl.ds(pl.multiple_of(half * rows, rows), rows)
    slabs_ = []
    for at, (source, target) in enumerate(
        ((w_hbm, own_w), (k_hbm, own_k), (v_hbm, own_v))
    ):
        copy = pltpu.make_async_copy(source, target, local_sem.at[8 + at])
        copy.start()
        slabs_.append(copy)
    locals_ = []
    for at, (source, target) in enumerate(zip(sources, targets)):
        copy = pltpu.make_async_copy(
            source.at[:, pl.ds(pl.multiple_of(half * width, PAIR), width)],
            target.at[mine, :],
            local_sem.at[at],
        )
        copy.start()
        locals_.append(copy)
    params = []
    for at, (source, target) in enumerate(
        ((bonus_hbm, bonus_ref), (gain_hbm, gain_ref), (bias_hbm, bias_ref))
    ):
        copy = pltpu.make_async_copy(source, target, local_sem.at[5 + at])
        copy.start()
        params.append(copy)
    def arrived(at):
        locals_[at].wait()
        for copy in remotes[at]:
            copy.wait_recv()

    lower = (
        lax.broadcasted_iota(jnp.int32, (rows, rows), 0)
        >= lax.broadcasted_iota(jnp.int32, (rows, rows), 1)
    ).astype(F32).astype(BF)
    lane = lax.broadcasted_iota(jnp.int32, (1, PAIR), 1)
    first_f = (lane < CHANNEL_COUNT).astype(F32)
    second_f = 1.0 - first_f
    first, second = first_f.astype(BF), second_f.astype(BF)
    at_row = lax.broadcasted_iota(jnp.int32, (2 * PAIR, PAIR), 0)
    at_lane = lax.broadcasted_iota(jnp.int32, (2 * PAIR, PAIR), 1)
    ones = (
        (lax.rem(at_row, PAIR) < CHANNEL_COUNT) == (at_lane < CHANNEL_COUNT)
    ).astype(F32).astype(BF)

    def head_sums(x):
        return dot(jnp.concatenate(split(x), axis=1), ones)

    for spare in range(pairs * groups, n * units):
        msg[spare // units, (spare % units) * ROWS : (spare % units + 1) * ROWS] = jnp.zeros(
            (ROWS, PAIR), F32
        )

    def spot(chunk, pair):
        return slice(chunk * rows, (chunk + 1) * rows), slice(pair * PAIR, (pair + 1) * PAIR)

    def summarize(hosted, pair):
        lanes = slice((hosted * pairs + pair) * PAIR, (hosted * pairs + pair + 1) * PAIR)
        cumul = dot(lower, own_w[:, lanes])
        final = cumul[rows - 1 : rows]
        center = 0.5 * final
        keys = split(own_k[:, lanes].astype(F32) * jnp.exp(center - cumul))
        full = dot_tn(own_v[:, lanes], jnp.concatenate(keys, axis=1))
        full = full[:, :PAIR] + full[:, PAIR:]
        ends = jnp.where(lane < CHANNEL_COUNT, full[:CHANNEL_COUNT], full[CHANNEL_COUNT:])
        ends_out[hosted, pair * CHANNEL_COUNT : (pair + 1) * CHANNEL_COUNT] = ends * jnp.exp(center)
        last = pairs * CHANNEL_COUNT + pair
        ends_out[hosted, last : last + 1] = jnp.exp(final)

    def combine(pair):
        lanes = slice(pair * PAIR, (pair + 1) * PAIR)
        state = total = None
        for chunk in range(heads):
            ends = ends_in[chunk, pair * CHANNEL_COUNT : (pair + 1) * CHANNEL_COUNT]
            last = pairs * CHANNEL_COUNT + pair
            step = ends_in[chunk, last : last + 1]
            if chunk == 0:
                state, total = ends, step
            else:
                small_ref[2 * chunk + 1 : 2 * chunk + 2, lanes] = total
                local_ref[chunk - 1, pair] = state
                state, total = step * state + ends, step * total
        for group in range(groups):
            unit = pair * groups + group
            to, slot = unit // units, unit % units
            msg[to, slot * ROWS : (slot + 1) * ROWS] = state[group * ROWS : (group + 1) * ROWS]
            msg[to, unit_rows + slot : unit_rows + slot + 1] = total

    def prepare(pair):
        for chunk in range(heads):
            at = spot(chunk, pair)
            decay = xw[at]
            cumul = dot(lower, decay)
            center = 0.5 * cumul[rows - 1 : rows]
            high, low = split(xq[at].astype(F32) * jnp.exp(cumul - decay.astype(F32) - center))
            rhi_ref[at], rlo_ref[at] = high, low
            high, low = split(xk[at].astype(F32) * jnp.exp(center - cumul))
            khi_ref[at], klo_ref[at] = high, low
            small_ref[2 * chunk : 2 * chunk + 1, at[1]] = jnp.exp(center)

    def within(pair):
        head = half * (width // CHANNEL_COUNT) + 2 * pair
        bonus = jnp.concatenate([bonus_ref[pl.ds(head, 1)], bonus_ref[pl.ds(head + 1, 1)]], axis=1)
        for chunk in range(heads):
            at = spot(chunk, pair)
            high, low = rhi_ref[at], rlo_ref[at]
            key_high, key_low, value = khi_ref[at], klo_ref[at], xv[at]
            keys = jnp.concatenate([key_high * first, key_high * second], axis=0)
            rest = jnp.concatenate([key_low * first, key_low * second], axis=0)
            scores = dot_nt(
                jnp.concatenate([high, low], axis=1), jnp.concatenate([keys, keys], axis=1)
            ) + dot_nt(high, rest)
            strict = lax.broadcasted_iota(jnp.int32, scores.shape, 0) > lax.rem(
                lax.broadcasted_iota(jnp.int32, scores.shape, 1), rows
            )
            scores = jnp.where(strict, scores, 0.0)
            values = jnp.concatenate([value * first, value * second], axis=0)
            both = dot(jnp.concatenate(split(scores), axis=0), values)
            diagonal = head_sums(xq[at].astype(F32) * bonus * xk[at].astype(F32))
            y_ref[at] = both[:rows] + both[rows:] + diagonal * value.astype(F32)

    def finish(pair):
        lanes = pl.ds(pl.multiple_of(half * width + pair * PAIR, PAIR), PAIR)
        gain, bias = gain_ref[lanes].reshape(1, PAIR), bias_ref[lanes].reshape(1, PAIR)
        pieces = []
        for group in range(groups):
            unit = pair * groups + group
            slot = unit % units
            pieces.append(carried[unit // units, slot * ROWS : (slot + 1) * ROWS])
        incoming = jnp.concatenate(pieces, axis=0)
        for chunk in range(heads):
            at = spot(chunk, pair)
            state = incoming
            if chunk > 0:
                total = small_ref[2 * chunk + 1 : 2 * chunk + 2, at[1]]
                state = total * incoming + local_ref[chunk - 1, pair]
            state = state * small_ref[2 * chunk : 2 * chunk + 1, at[1]]
            state_high, state_low = split(
                jnp.concatenate([state * first_f, state * second_f], axis=0)
            )
            high, low = rhi_ref[at], rlo_ref[at]
            y = (
                y_ref[at]
                + dot_nt(
                    jnp.concatenate([high, low], axis=1),
                    jnp.concatenate([state_high, state_high], axis=1),
                )
                + dot_nt(high, state_low)
            )
            y = y - head_sums(y) * (1.0 / CHANNEL_COUNT)
            spread = head_sums(y * y) * (1.0 / CHANNEL_COUNT)
            normed = y * lax.rsqrt(spread + 1e-05)
            gate = xg[at].astype(F32)
            gated = (normed * gain + bias) * (gate / (1.0 + jnp.exp(-gate)))
            out_ref[at] = gated.astype(out_ref.dtype)

    def outgoing(peer):
        return pltpu.make_async_remote_copy(
            src_ref=msg.at[peer],
            dst_ref=inbox.at[me],
            send_sem=send1.at[peer],
            recv_sem=recv1.at[me],
            device_id=(peer, half),
            device_id_type=MESH,
        )

    def incoming_from(peer):
        return pltpu.make_async_remote_copy(
            src_ref=msg.at[peer],
            dst_ref=inbox.at[peer],
            send_sem=send1.at[peer],
            recv_sem=recv1.at[peer],
            device_id=(peer, half),
            device_id_type=MESH,
        )

    def back_to(peer):
        return pltpu.make_async_remote_copy(
            src_ref=prefix.at[peer],
            dst_ref=carried.at[me],
            send_sem=send2.at[peer],
            recv_sem=recv2.at[me],
            device_id=(peer, half),
            device_id_type=MESH,
        )

    def back_from(peer):
        return pltpu.make_async_remote_copy(
            src_ref=prefix.at[peer],
            dst_ref=carried.at[peer],
            send_sem=send2.at[peer],
            recv_sem=recv2.at[peer],
            device_id=(peer, half),
            device_id_type=MESH,
        )

    def others(act):
        def body(step, carry):
            act(lax.rem(me + step, n))
            return carry

        lax.fori_loop(1, n, body, 0)

    for copy in slabs_:
        copy.wait()
    for spare in range(pairs, ends_out.shape[1] - pairs * CHANNEL_COUNT):
        for hosted in range(heads):
            last = pairs * CHANNEL_COUNT + spare
            ends_out[hosted, last : last + 1] = jnp.zeros((1, PAIR), F32)
    for hosted in range(heads):
        for pair in range(pairs):
            summarize(hosted, pair)
    pl.semaphore_wait(barrier, n - 1 + heads - 1)
    swaps = []
    for step in range(1, heads):
        other = lax.rem(half + step, heads)
        copy = pltpu.make_async_remote_copy(
            src_ref=ends_out.at[other],
            dst_ref=ends_in.at[half],
            send_sem=esend.at[step - 1],
            recv_sem=erecv.at[step - 1],
            device_id=(me, other),
            device_id_type=MESH,
        )
        copy.start()
        swaps.append(copy)
    remotes = []
    for at, (source, target) in enumerate(zip(sources, targets)):
        group = []
        for step in range(1, heads):
            other = lax.rem(half + step, heads)
            copy = pltpu.make_async_remote_copy(
                src_ref=source.at[:, pl.ds(pl.multiple_of(other * width, PAIR), width)],
                dst_ref=target.at[mine, :],
                send_sem=hsend.at[at, step - 1],
                recv_sem=hrecv.at[at, step - 1],
                device_id=(me, other),
                device_id_type=MESH,
            )
            copy.start()
            group.append(copy)
        remotes.append(group)

    ends_in[half] = ends_out[half]
    for copy in swaps:
        copy.wait_recv()
    for pair in range(pairs):
        combine(pair)
    others(lambda peer: outgoing(peer).start())
    for copy in params:
        copy.wait()
    inbox[me] = msg[me]
    for at in range(4):
        arrived(at)
    early = pairs // 2
    for pair in range(early):
        prepare(pair)
        within(pair)

    def scan(source, state):
        prefix[source] = state

        @pl.when(source != me)
        def _():
            back_to(source).start()

        @pl.when(source == me)
        def _():
            carried[source] = state

        @pl.when(source != me)
        def _():
            incoming_from(source).wait_recv()

        block = inbox[source]
        parts = []
        for slot in range(units):
            rows_of = slice(slot * ROWS, (slot + 1) * ROWS)
            decay = block[unit_rows + slot : unit_rows + slot + 1]
            parts.append(state[rows_of] * decay + block[rows_of])
        return jnp.concatenate(parts, axis=0) if units > 1 else parts[0]

    lax.fori_loop(0, n, scan, jnp.zeros((unit_rows, PAIR), F32))
    for pair in range(early, pairs):
        prepare(pair)
        within(pair)
    arrived(4)

    def home(owner):
        @pl.when(owner != me)
        def _():
            back_from(owner).wait_recv()

    ready = 0
    for pair in range(pairs):
        needed = (pair * groups + groups - 1) // units + 1
        for owner in range(ready, needed):
            home(owner)
        ready = needed
        finish(pair)
    for owner in range(ready, n):
        home(owner)
    for copy in swaps:
        copy.wait_send()
    for group in remotes:
        for copy in group:
            copy.wait_send()
    others(lambda peer: outgoing(peer).wait_send())
    others(lambda peer: back_to(peer).wait_send())


def solution(mesh):
    n, heads = mesh.shape["seq"], mesh.shape["head"]

    def body(q, k, v, w, g, bonus, gain, bias):
        rows, full = q.shape
        width = full // heads
        length = rows * heads
        pairs = width // PAIR
        units = -(-pairs * (CHANNEL_COUNT // ROWS) // n)
        unit_rows = units * ROWS
        end_rows = pairs * CHANNEL_COUNT + -(-pairs // ROWS) * ROWS
        message_rows = unit_rows + -(-units // ROWS) * ROWS
        anywhere = pl.BlockSpec(memory_space=pltpu.HBM)
        inside = pl.BlockSpec(memory_space=pltpu.VMEM)
        dma = pltpu.SemaphoreType.DMA
        slab = (length, width)
        return pl.pallas_call(
            functools.partial(kernel, n, heads, units),
            out_shape=jax.ShapeDtypeStruct(slab, jnp.bfloat16),
            in_specs=[anywhere] * 8,
            out_specs=inside,
            scratch_shapes=[pltpu.VMEM(bonus.shape, F32)]
            + [pltpu.VMEM((full,), F32)] * 2
            + [pltpu.VMEM(slab, BF)] * 5
            + [pltpu.VMEM((rows, full), BF)] * 3
            + [pltpu.VMEM((heads, end_rows, PAIR), F32)] * 2
            + [pltpu.VMEM(slab, BF)] * 4
            + [
                pltpu.VMEM(slab, F32),
                pltpu.VMEM((max(heads - 1, 1), pairs, CHANNEL_COUNT, PAIR), F32),
                pltpu.VMEM((2 * heads, width), F32),
                pltpu.VMEM((n, message_rows, PAIR), F32),
                pltpu.VMEM((n, message_rows, PAIR), F32),
                pltpu.VMEM((n, unit_rows, PAIR), F32),
                pltpu.VMEM((n, unit_rows, PAIR), F32),
                dma((11,)),
                dma((max(heads - 1, 1),)),
                dma((max(heads - 1, 1),)),
                dma((5, max(heads - 1, 1))),
                dma((5, max(heads - 1, 1))),
                dma((n,)),
                dma((n,)),
                dma((n,)),
                dma((n,)),
            ],
            compiler_params=pltpu.CompilerParams(
                collective_id=0, has_side_effects=True, vmem_limit_bytes=60 * 1024 * 1024
            ),
        )(q, k, v, w, g, bonus, gain, bias)

    slabs = P(("seq", "head"), None)
    return jax.shard_map(
        body,
        mesh=mesh,
        in_specs=(slabs,) * 5 + (P(), P(), P()),
        out_specs=P("seq", "head"),
        check_vma=False,
    )
```
